32 devices in a mesh: span: 8 (over z, y), depth: 4 (over x, core).
Axes of the slice: x: 2, y: 2, z: 4, core: 2. Of those that a mesh axis runs over, the one named last changes fastest.
Arguments:
- part_slab: int32 [4, 65536, 1], P('depth', 'span'), may hold values from 0 to 7; in each aligned block of 8192 rows (0 to 8191, 8192 to 16383, ..., all dimensions but the last counted through in order) at most 2048 rows name the same one
- part_cell: int32 [4, 65536], P('depth', 'span'), may hold values from 0 to 65535
- part_volume: float32 [4, 65536], P('depth', 'span'), may hold values from 0.05 to 0.6
- part_drag: float32 [3, 4, 65536], P(None, 'depth', 'span'), may hold values from -6 to 6
- part_count: int32 [4, 8], P('depth', 'span'), may hold values from 7168 to 8192
- prior_solid: float32 [8, 128, 2048], P(None, 'span', 'depth'), may hold values from 0 to 0.6
- prior_drag: float32 [3, 8, 128, 2048], P(None, None, 'span', 'depth'), may hold values from -4 to 4
Outputs:
- fields: float32 [4, 8, 128, 2048], P(None, None, 'span', 'depth')
- feedback: float32 [4, 4, 65536], P(None, 'depth', 'span')
The draws below stay inside these ranges and needn't reach their ends.
Inputs may be any that keep to these rules, and one draw needn't show every extreme that they name: `part_slab`: among the 8192 particle slots of one owner device, live or not, no slab is named more than 2048 times; in every draw some device names a slab exactly 2048 times.
All inputs are finite; a program needn't handle non-finite values.
Results may differ from the reference program's by a relative error of at most 0.0003.
Values sent between devices are 32-bit elements; how exact they have to be, the bound alone decides.
A program may use at most 128 MiB of HBM per device.

```python
import math
import jax
import jax.numpy as jnp
import numpy as np

CX = 16
CY = 512
LAYERS = 8
SWEEPS = 6
PART_DEV = 8192
CAP = 2048
NX = 128
NY = 2048
SPAN_PARTS = 65536
N_SPAN = 8
N_DEPTH = 4


def with_ends(entries, own_key, low, top_value):
    spot = [jax.random.randint(jax.random.fold_in(own_key, axis), (), 0, length) for axis, length in enumerate(entries.shape)]
    longest = entries.shape.index(max(entries.shape))
    next_to = spot[:longest] + [(spot[longest] + 1) % entries.shape[longest]] + spot[longest + 1:]
    return entries.at[tuple(spot)].set(low).at[tuple(next_to)].set(top_value)


def levels(stream_key, extent, split, least, high):
    factor_of, own = 1.0, jax.random.fold_in(stream_key, 6)
    for axis_at, shards_of in split:
        draws = jnp.exp(jax.random.uniform(jax.random.fold_in(own, axis_at), (shards_of,), jnp.float32, least / len(split), high / len(split)))
        factor_of = factor_of * jnp.repeat(draws, extent[axis_at] // shards_of).reshape([-1 if axis == axis_at else 1 for axis in range(len(extent))])
    return factor_of


def deal_out(key, own, number, rows, number_of, top, most, skew):
    ranking = jax.random.permutation(key, number_of)
    crowded, usual = portions_of(number_of, rows * top, most, skew, True), portions_of(number_of, rows * top, most, skew, False)
    places = jnp.arange(number_of)

    def named(lengths, rotation):
        used = int((lengths > 0).sum())
        fixed = max(1, used // 4)
        passed = fixed + (places - fixed + rotation * (used - fixed)) % max(1, number_of - fixed)
        return jnp.zeros((number_of,), jnp.int32).at[ranking[jnp.where(places < fixed, places, passed)]].set(jnp.asarray(lengths, jnp.int32))

    lengths = jnp.where(number % 4 == 0, named(crowded, number // 4), named(usual, number - number // 4 - 1))
    mixed = jax.random.permutation(jax.random.fold_in(own, 3), number_of)
    giver, receiver = mixed[0:number_of // 2 * 2:2], mixed[1:number_of // 2 * 2:2]
    room = jnp.minimum(lengths[giver] - 1, most - lengths[receiver]) // 2
    room = jnp.where((giver == ranking[0]) | (receiver == ranking[0]) | (lengths[receiver] == 0), 0, jnp.maximum(room, 0))
    passed = jax.random.randint(jax.random.fold_in(own, 4), (number_of // 2,), 0, 1 << 20) % (room + 1)
    lengths = lengths.at[giver].add(-passed).at[receiver].add(passed)
    labels = jnp.searchsorted(jnp.cumsum(lengths), jnp.arange(rows * top), side="right").astype(jnp.int32)
    table = labels.reshape(top, rows).T
    table = table[jax.random.permutation(jax.random.fold_in(own, 1), rows)]
    rotation = jax.random.randint(jax.random.fold_in(own, 2), (rows, 1), 0, top)
    return jnp.take_along_axis(table, (jnp.arange(top)[None, :] + rotation) % top, axis=1)


def portions_of(number_of, total, most, lean, full):
    portions = [(1 << 20) // math.isqrt(grade ** lean) + 1 for grade in range(1, number_of + 1)]
    largest = most if full else min(most, max(-(-total // number_of), total * portions[0] // sum(portions)))
    least = 1 if total - largest >= number_of - 1 else 0
    holding, rest = [largest] + [least] * (number_of - 1), total - largest - least * (number_of - 1)
    while rest > 0:
        free = [i for i in range(1, number_of) if holding[i] < largest] or [i for i in range(1, number_of) if holding[i] < most]
        mass, remaining = sum([portions[i] for i in free]), rest
        for i in free:
            more = min(most - holding[i], max(1, remaining * portions[i] // mass), rest)
            holding[i] = holding[i] + more
            rest = rest - more
    return np.array(holding)


def normal_values(stream_key, dims, scale, bound, pieces=(), held_as=jnp.bfloat16):
    values = jax.random.normal(stream_key, dims, jnp.float32) * scale
    if len(pieces) > 0:
        values = levels(stream_key, dims, pieces, -0.22, 0.18) * values
    return jnp.clip(values, min=-bound, max=bound).astype(held_as)


def setup_inputs(seed: int = 0) -> dict:
    key_of = jax.random.split(jax.random.key(seed), 8)
    part_slab_keys = jax.random.split(jax.random.fold_in(key_of[0], 1), N_DEPTH * SPAN_PARTS // PART_DEV)
    part_slab_turns = jax.random.permutation(jax.random.fold_in(key_of[0], 3), N_DEPTH * SPAN_PARTS // PART_DEV)
    part_slab = jax.vmap(lambda own, number: deal_out(jax.random.fold_in(key_of[0], 2), own, number, PART_DEV, N_SPAN, 1, CAP, 2))(part_slab_keys, part_slab_turns).reshape((N_DEPTH, SPAN_PARTS, 1))
    part_cell = with_ends(jax.random.randint(key_of[1], (N_DEPTH, SPAN_PARTS), 0, LAYERS * CX * CY), jax.random.fold_in(key_of[1], 1), 0, (LAYERS * CX * CY) - 1).astype(jnp.int32)
    part_volume = jnp.clip(jnp.exp(math.log(0.6) - 2.4849067 * jax.random.uniform(key_of[2], (N_DEPTH, SPAN_PARTS), jnp.float32) ** levels(key_of[2], (N_DEPTH, SPAN_PARTS), ((0, 4), (1, 8)), -0.2, 0.2)), 0.05, 0.6)
    part_drag = normal_values(key_of[3], (3, N_DEPTH, SPAN_PARTS), 1.0, 6.0, ((1, 4), (2, 8)), jnp.float32)
    part_count = with_ends(jax.random.randint(key_of[4], (N_DEPTH, N_SPAN), PART_DEV * 7 // 8, PART_DEV + 1), jax.random.fold_in(key_of[4], 1), PART_DEV * 7 // 8, PART_DEV).astype(jnp.int32)
    prior_solid = jnp.clip(0.6 * jax.random.uniform(key_of[5], (LAYERS, NX, NY), jnp.float32) ** levels(key_of[5], (LAYERS, NX, NY), ((1, 8), (2, 4)), -0.2, 0.2), 0.0, 0.6)
    prior_drag = normal_values(key_of[6], (3, LAYERS, NX, NY), 0.5, 4.0, ((2, 8), (3, 4)), jnp.float32)
    return dict(part_slab=part_slab, part_cell=part_cell, part_volume=part_volume, part_drag=part_drag, part_count=part_count, prior_solid=prior_solid, prior_drag=prior_drag)


NU_WEIGHT = 1.0
PHI_LIMIT = 0.6


def relax_once(source, padded):
    beside = padded[:, :, 2:, 1:-1] + padded[:, :, :-2, 1:-1]
    beside = beside + padded[:, :, 1:-1, 2:] + padded[:, :, 1:-1, :-2]
    return (source + NU_WEIGHT * beside) / (1.0 + 4.0 * NU_WEIGHT)


def reference(part_slab, part_cell, part_volume, part_drag, part_count, prior_solid, prior_drag):
    depth_count = part_cell.shape[0]
    span_rows = part_cell.shape[1]
    grid_x = CX * N_SPAN
    grid_y = CY * N_DEPTH
    slab_index = part_slab[:, :, 0]
    column = jnp.arange(span_rows, dtype=jnp.int32)
    owner_index = column // PART_DEV
    within = column % PART_DEV
    counts = part_count[:, owner_index]
    live_weight = (within[None, :] < counts).astype(jnp.float32)
    layer_index = part_cell // (CX * CY)
    local_x = (part_cell // CY) % CX
    local_y = part_cell % CY
    depth_row = jnp.arange(depth_count, dtype=jnp.int32)[:, None]
    flat_index = layer_index * (grid_x * grid_y) + (slab_index * CX + local_x) * grid_y + depth_row * CY + local_y
    flat_index = flat_index.astype(jnp.int32).reshape(-1)
    payload = jnp.concatenate([part_volume[None], part_drag], axis=0) * live_weight[None]
    deposit = jax.ops.segment_sum(payload.reshape(4, -1).T, flat_index, num_segments=LAYERS * grid_x * grid_y)
    deposit = deposit.T.reshape(4, LAYERS, grid_x, grid_y)
    target = jnp.concatenate([jnp.minimum(deposit[:1], PHI_LIMIT), deposit[1:]], axis=0)
    smooth = jnp.concatenate([prior_solid[None], prior_drag], axis=0)
    for sweep_index in range(SWEEPS):
        padded = jnp.pad(smooth, ((0, 0), (0, 0), (1, 1), (1, 1)))
        smooth = relax_once(target, padded)
    void_fraction = 1.0 - smooth[0]
    fields = jnp.concatenate([void_fraction[None], -smooth[1:] / void_fraction[None]], axis=0)
    feedback = fields.reshape(4, -1)[:, flat_index].reshape(4, depth_count, span_rows) * live_weight[None]
    return (fields, feedback)
```

```python
import functools
import math

import jax
import jax.numpy as jnp
from jax import lax
from jax.experimental import pallas as pl
from jax.experimental.pallas import tpu as pltpu
from jax.sharding import PartitionSpec as P

SWEEPS = 6
NU_WEIGHT = 1.0
PHI_LIMIT = 0.6
BF = jnp.bfloat16
F32 = jnp.float32


def two_parts(value):
    high = value.astype(BF)
    return high, (value - high.astype(F32)).astype(BF)


def hot_of(index, count):
    rows = lax.broadcasted_iota(jnp.int32, (count, index.shape[1]), 0)
    return jnp.where(rows == index, 1.0, 0.0).astype(BF)


def nt_dot(left, right):
    return lax.dot_general(left, right, (((1,), (1,)), ((), ())), preferred_element_type=F32)


def spread(values, row, col, rows, cols):
    mask = lax.broadcasted_iota(jnp.int32, (rows, row.shape[1]), 0) == row
    hot = hot_of(col, cols)
    total = None
    for part in range(2):
        left = jnp.concatenate(
            [jnp.where(mask, two_parts(v)[part].astype(F32), 0.0).astype(BF) for v in values], axis=0
        )
        term = nt_dot(left, hot)
        total = term if total is None else total + term
    return total


def pick(high, low, row, col, rows, cols):
    hot = hot_of(col, cols)
    wide = jnp.dot(high, hot, preferred_element_type=F32)
    wide = wide + jnp.dot(low, hot, preferred_element_type=F32)
    mask = lax.broadcasted_iota(jnp.int32, (rows, row.shape[1]), 0) == row
    comps = high.shape[0] // rows
    found = [
        jnp.sum(jnp.where(mask, wide[c * rows : (c + 1) * rows], 0.0), axis=0, keepdims=True)
        for c in range(comps)
    ]
    return found


def pack_kernel(span, cap, block, count, slab, cell, volume, drag, out, slots):
    rows, cols = out.shape[1:]
    part_rows = slab.shape[1]
    out[...] = jnp.zeros_like(out)
    before_lane = lax.broadcasted_iota(jnp.int32, (block, block), 0)
    this_lane = lax.broadcasted_iota(jnp.int32, (block, block), 1)
    tri = jnp.where(before_lane < this_lane, 1.0, 0.0).astype(BF)
    live_count = count[0, 0]

    def step(b, offset):
        lanes = pl.ds(pl.multiple_of(b * block, block), block)
        sl = slab[:, lanes]
        live = b * block + lax.broadcasted_iota(jnp.int32, (1, block), 1) < live_count
        key = jnp.where(live, sl, -1)
        member = jnp.where(lax.broadcasted_iota(jnp.int32, (span, block), 0) == key, 1.0, 0.0)
        before = jnp.dot(member.astype(BF), tri, preferred_element_type=F32)
        place = jnp.sum(member * (before + offset), axis=0, keepdims=True).astype(jnp.int32)
        slot = jnp.where(live, sl * cap + place, -1)
        slots[:, lanes] = slot
        row = lax.shift_right_arithmetic(slot, int(math.log2(cols)))
        col = lax.bitwise_and(slot, cols - 1)
        values = [cell[:, lanes].astype(F32), volume[:, lanes]]
        values += [drag[c, :, lanes] for c in range(drag.shape[0])]
        out[...] += spread(values, row, col, rows, cols).reshape(out.shape)
        return offset + jnp.sum(member, axis=1, keepdims=True)

    lax.fori_loop(0, part_rows // block, step, jnp.zeros((span, 1), F32))


def deposit_kernel(group, recv, out):
    comps, rows, cols = out.shape
    out[...] = jnp.zeros_like(out)

    def step(g, carry):
        lines = pl.ds(pl.multiple_of(g * group, group), group)
        block = [recv[c, lines, :] for c in range(comps + 1)]
        flat = [
            jnp.concatenate([b[j : j + 1] for j in range(group)], axis=1) for b in block
        ]
        ids = flat[0].astype(jnp.int32)
        row = lax.shift_right_arithmetic(ids, int(math.log2(cols)))
        col = lax.bitwise_and(ids, cols - 1)
        out[...] += spread(flat[1:], row, col, rows, cols).reshape(out.shape)
        return carry

    lax.fori_loop(0, recv.shape[1] // group, step, 0)
    out[0] = jnp.minimum(out[0], PHI_LIMIT)


def gather_kernel(group, fields, ids_ref, out, high, low):
    comps, rows, cols = fields.shape
    table = fields[...].reshape(comps * rows, cols)
    high[...], low[...] = two_parts(table)

    def step(g, carry):
        lines = pl.ds(pl.multiple_of(g * group, group), group)
        block = ids_ref[0, lines, :].astype(jnp.int32)
        found = []
        for j in range(group):
            ids = block[j : j + 1]
            row = lax.shift_right_arithmetic(ids, int(math.log2(cols)))
            col = lax.bitwise_and(ids, cols - 1)
            found.append(pick(high[...], low[...], row, col, rows, cols))
        for c in range(comps):
            out[c, lines, :] = jnp.concatenate([f[c] for f in found], axis=0)
        return carry

    lax.fori_loop(0, ids_ref.shape[1] // group, step, 0)


def unpack_kernel(block, table_ref, slots, out):
    comps, rows, cols = table_ref.shape
    high, low = two_parts(table_ref[...].reshape(comps * rows, cols))

    def step(b, carry):
        lanes = pl.ds(pl.multiple_of(b * block, block), block)
        slot = slots[:, lanes]
        row = lax.shift_right_arithmetic(slot, int(math.log2(cols)))
        col = lax.bitwise_and(slot, cols - 1)
        found = pick(high, low, row, col, rows, cols)
        for c in range(comps):
            out[c, :, lanes] = found[c]
        return carry

    lax.fori_loop(0, slots.shape[1] // block, step, 0)


def padded_2(array, sides, width):
    for axis, dim in sides:
        count, length = (lax.axis_size(axis), array.shape[dim])
        up = [(i, (i + 1) % count) for i in range(count - 1)]
        down = [(j, i) for i, j in up]
        last = lax.slice_in_dim(array, length - width, length, axis=dim)
        first = lax.slice_in_dim(array, 0, width, axis=dim)
        before = lax.ppermute(last, axis, up)
        after = lax.ppermute(first, axis, down)
        array = jnp.concatenate([before, array, after], axis=dim)
    return array


def relax_once(source, padded):
    beside = padded[:, :, 2:, 1:-1] + padded[:, :, :-2, 1:-1]
    beside = beside + padded[:, :, 1:-1, 2:] + padded[:, :, 1:-1, :-2]
    return (source + NU_WEIGHT * beside) / (1.0 + 4.0 * NU_WEIGHT)


VMEM = pl.BlockSpec(memory_space=pltpu.VMEM)
SMEM = pl.BlockSpec(memory_space=pltpu.SMEM)
LIMIT = pltpu.CompilerParams(vmem_limit_bytes=48 * 1024 * 1024)


def on_device(part_slab, part_cell, part_volume, part_drag, part_count, prior_solid, prior_drag):
    span_size = lax.axis_size("span")
    depth_size = lax.axis_size("depth")
    part_rows = part_cell.shape[1]
    cap = 2 * part_rows // span_size
    layers, width_x, width_y = prior_solid.shape
    cols = min(256, cap)
    lines = span_size * cap // cols
    block = math.gcd(part_rows, 512)
    packed, slots = pl.pallas_call(
        functools.partial(pack_kernel, span_size, cap, block),
        out_shape=(
            jax.ShapeDtypeStruct((5, lines, cols), F32),
            jax.ShapeDtypeStruct((1, part_rows), jnp.int32),
        ),
        in_specs=[SMEM] + [VMEM] * 4,
        out_specs=(VMEM, VMEM),
        compiler_params=LIMIT,
        name="pack",
    )(part_count, part_slab.reshape(1, part_rows), part_cell, part_volume, part_drag)
    per = lines // span_size
    recv = lax.all_to_all(
        packed.reshape(5, span_size, per, cols), "span", split_axis=1, concat_axis=1, tiled=True
    ).reshape(5, lines, cols)
    grid_rows = layers * width_x
    target = pl.pallas_call(
        functools.partial(deposit_kernel, 8),
        out_shape=jax.ShapeDtypeStruct((4, grid_rows, width_y), F32),
        in_specs=[VMEM],
        out_specs=VMEM,
        compiler_params=LIMIT,
        name="deposit",
    )(recv)
    target = target.reshape(4, layers, width_x, width_y)
    smooth = jnp.concatenate([prior_solid[None], prior_drag], axis=0)
    rim_width = 3
    row_ids = (
        lax.axis_index("span") * width_x
        - rim_width
        + jnp.arange(width_x + 2 * rim_width, dtype=jnp.int32)
    )
    col_ids = (
        lax.axis_index("depth") * width_y
        - rim_width
        + jnp.arange(width_y + 2 * rim_width, dtype=jnp.int32)
    )
    row_inside = (row_ids >= 0) & (row_ids < span_size * width_x)
    col_inside = (col_ids >= 0) & (col_ids < depth_size * width_y)
    inside = (row_inside[:, None] & col_inside[None, :]).astype(jnp.float32)
    stacked = padded_2(
        jnp.concatenate([smooth, target], axis=0), (("span", 2), ("depth", 3)), rim_width
    )
    padded = stacked[:4]
    target_wide = stacked[4:]
    for round_index in range(SWEEPS // rim_width):
        if round_index > 0:
            padded = padded_2(smooth, (("span", 2), ("depth", 3)), rim_width)
        for inner_step in range(rim_width):
            edge_offset = inner_step + 1
            size_x = width_x + 2 * (rim_width - edge_offset)
            size_y = width_y + 2 * (rim_width - edge_offset)
            region = target_wide[
                :, :, edge_offset : edge_offset + size_x, edge_offset : edge_offset + size_y
            ]
            keeper = inside[edge_offset : edge_offset + size_x, edge_offset : edge_offset + size_y]
            padded = relax_once(region, padded) * keeper[None, None]
        smooth = padded
    void_fraction = 1.0 - smooth[0]
    fields = jnp.concatenate([void_fraction[None], -smooth[1:] / void_fraction[None]], axis=0)
    table = fields.reshape(4, grid_rows, width_y)
    values = pl.pallas_call(
        functools.partial(gather_kernel, 8),
        out_shape=jax.ShapeDtypeStruct((4, lines, cols), F32),
        in_specs=[VMEM] * 2,
        out_specs=VMEM,
        scratch_shapes=[pltpu.VMEM((4 * grid_rows, width_y), BF)] * 2,
        compiler_params=LIMIT,
        name="gather",
    )(table, recv)
    returned = lax.all_to_all(
        values.reshape(4, span_size, per, cols), "span", split_axis=1, concat_axis=1, tiled=True
    ).reshape(4, lines, cols)
    feedback = pl.pallas_call(
        functools.partial(unpack_kernel, block),
        out_shape=jax.ShapeDtypeStruct((4, 1, part_rows), F32),
        in_specs=[VMEM] * 2,
        out_specs=VMEM,
        compiler_params=LIMIT,
        name="unpack",
    )(returned, slots)
    return (fields, feedback)


def solution(mesh):
    in_specs = (
        P("depth", "span", None),
        P("depth", "span"),
        P("depth", "span"),
        P(None, "depth", "span"),
        P("depth", "span"),
        P(None, "span", "depth"),
        P(None, None, "span", "depth"),
    )
    out_specs = (P(None, None, "span", "depth"), P(None, "depth", "span"))
    return jax.shard_map(
        on_device, mesh=mesh, in_specs=in_specs, out_specs=out_specs, check_vma=False
    )
```

```python
import functools
import math

import jax
import jax.numpy as jnp
from jax import lax
from jax.experimental import pallas as pl
from jax.experimental.pallas import tpu as pltpu
from jax.sharding import PartitionSpec as P

SWEEPS = 6
NU_WEIGHT = 1.0
PHI_LIMIT = 0.6
BF = jnp.bfloat16
F32 = jnp.float32


def two_parts(value):
    high = value.astype(BF)
    return high, (value - high.astype(F32)).astype(BF)


def hot_of(index, count):
    rows = lax.broadcasted_iota(jnp.int32, (count, index.shape[1]), 0)
    return jnp.where(rows == index, 1.0, 0.0).astype(BF)


def nt_dot(left, right):
    return lax.dot_general(left, right, (((1,), (1,)), ((), ())), preferred_element_type=F32)


def spread(values, row, col, rows, cols):
    mask = lax.broadcasted_iota(jnp.int32, (rows, row.shape[1]), 0) == row
    hot = hot_of(col, cols)
    total = None
    for part in range(2):
        left = jnp.concatenate(
            [jnp.where(mask, two_parts(v)[part].astype(F32), 0.0).astype(BF) for v in values], axis=0
        )
        term = nt_dot(left, hot)
        total = term if total is None else total + term
    return total


def pick(high, low, row, col, rows, cols):
    hot = hot_of(col, cols)
    wide = jnp.dot(high, hot, preferred_element_type=F32)
    wide = wide + jnp.dot(low, hot, preferred_element_type=F32)
    mask = lax.broadcasted_iota(jnp.int32, (rows, row.shape[1]), 0) == row
    comps = high.shape[0] // rows
    found = [
        jnp.sum(jnp.where(mask, wide[c * rows : (c + 1) * rows], 0.0), axis=0, keepdims=True)
        for c in range(comps)
    ]
    return found


def pack_kernel(span, cap, block, count, slab, cell, volume, drag, out, slots):
    rows, cols = out.shape[1:]
    part_rows = slab.shape[1]
    out[...] = jnp.zeros_like(out)
    before_lane = lax.broadcasted_iota(jnp.int32, (block, block), 0)
    this_lane = lax.broadcasted_iota(jnp.int32, (block, block), 1)
    tri = jnp.where(before_lane < this_lane, 1.0, 0.0).astype(BF)
    live_count = count[0, 0]

    def step(b, offset):
        lanes = pl.ds(pl.multiple_of(b * block, block), block)
        sl = slab[:, lanes]
        live = b * block + lax.broadcasted_iota(jnp.int32, (1, block), 1) < live_count
        key = jnp.where(live, sl, -1)
        member = jnp.where(lax.broadcasted_iota(jnp.int32, (span, block), 0) == key, 1.0, 0.0)
        before = jnp.dot(member.astype(BF), tri, preferred_element_type=F32)
        place = jnp.sum(member * (before + offset), axis=0, keepdims=True).astype(jnp.int32)
        slot = jnp.where(live, sl * cap + place, -1)
        slots[:, lanes] = slot
        row = lax.shift_right_arithmetic(slot, int(math.log2(cols)))
        col = lax.bitwise_and(slot, cols - 1)
        values = [cell[:, lanes].astype(F32), volume[:, lanes]]
        values += [drag[c, :, lanes] for c in range(drag.shape[0])]
        out[...] += spread(values, row, col, rows, cols).reshape(out.shape)
        return offset + jnp.sum(member, axis=1, keepdims=True)

    lax.fori_loop(0, part_rows // block, step, jnp.zeros((span, 1), F32))


def x_major(ids, layers, width_x, cols):
    line = lax.shift_right_arithmetic(ids, int(math.log2(cols)))
    layer = lax.shift_right_arithmetic(line, int(math.log2(width_x)))
    return lax.bitwise_and(line, width_x - 1) * layers + layer


def deposit_kernel(group, layers, recv, out):
    comps, rows, cols = out.shape
    out[...] = jnp.zeros_like(out)

    def step(g, carry):
        lines = pl.ds(pl.multiple_of(g * group, group), group)
        block = [recv[c, lines, :] for c in range(comps + 1)]
        flat = [
            jnp.concatenate([b[j : j + 1] for j in range(group)], axis=1) for b in block
        ]
        ids = flat[0].astype(jnp.int32)
        row = x_major(ids, layers, rows // layers, cols)
        col = lax.bitwise_and(ids, cols - 1)
        out[...] += spread(flat[1:], row, col, rows, cols).reshape(out.shape)
        return carry

    lax.fori_loop(0, recv.shape[1] // group, step, 0)
    out[0] = jnp.minimum(out[0], PHI_LIMIT)


def gather_kernel(group, smooth, ids_ref, fields, out, high, low):
    comps, width_x, layers, cols = smooth.shape
    rows = width_x * layers
    for x in range(width_x):
        void = 1.0 - smooth[0, x]
        for c in range(comps):
            value = void if c == 0 else -smooth[c, x] / void
            fields[c, :, x, :] = value
            lines = pl.ds(c * rows + x * layers, layers)
            high[lines], low[lines] = two_parts(value)

    def step(g, carry):
        lines = pl.ds(pl.multiple_of(g * group, group), group)
        block = ids_ref[0, lines, :].astype(jnp.int32)
        found = []
        for j in range(group):
            ids = block[j : j + 1]
            row = x_major(ids, layers, width_x, cols)
            col = lax.bitwise_and(ids, cols - 1)
            found.append(pick(high[...], low[...], row, col, rows, cols))
        for c in range(comps):
            out[c, lines, :] = jnp.concatenate([f[c] for f in found], axis=0)
        return carry

    lax.fori_loop(0, ids_ref.shape[1] // group, step, 0)


def unpack_kernel(block, table_ref, slots, out):
    comps, rows, cols = table_ref.shape
    high, low = two_parts(table_ref[...].reshape(comps * rows, cols))

    def step(b, carry):
        lanes = pl.ds(pl.multiple_of(b * block, block), block)
        slot = slots[:, lanes]
        row = lax.shift_right_arithmetic(slot, int(math.log2(cols)))
        col = lax.bitwise_and(slot, cols - 1)
        found = pick(high, low, row, col, rows, cols)
        for c in range(comps):
            out[c, :, lanes] = found[c]
        return carry

    lax.fori_loop(0, slots.shape[1] // block, step, 0)


MESH = pl.DeviceIdType.MESH
NEAR = [(dx, dy) for dx in (-1, 0, 1) for dy in (-1, 0, 1) if (dx, dy) != (0, 0)]


def sweeps_kernel(rim, solid, drag, target, out, smooth, source, ysend, yrecv, send_sem, recv_sem):
    comps, width_x, layers, width_y = target.shape
    span, depth = lax.axis_index("span"), lax.axis_index("depth")
    span_size, depth_size = lax.axis_size("span"), lax.axis_size("depth")
    own = pl.ds(128, width_y)
    total_x = width_x + 2 * rim

    def has(dx, dy):
        x, y = span + dx, depth + dy
        return (x >= 0) & (x < span_size) & (y >= 0) & (y < depth_size)

    barrier = pltpu.get_barrier_semaphore()
    for dx, dy in NEAR:

        @pl.when(has(dx, dy))
        def _(dx=dx, dy=dy):
            pl.semaphore_signal(
                barrier, inc=1, device_id=(span + dx, depth + dy), device_id_type=MESH
            )

    buffers = (smooth, source)

    def copy_of(which, at):
        dx, dy = NEAR[at]
        width = rim - which
        buffer = buffers[which]
        if dy == 0 and dx == 1:
            src = buffer.at[:, pl.ds(width_x + rim - width, width), :, own]
            dst = buffer.at[:, pl.ds(rim - width, width), :, own]
        elif dy == 0:
            src = buffer.at[:, pl.ds(rim, width), :, own]
            dst = buffer.at[:, pl.ds(width_x + rim, width), :, own]
        else:
            side = (dy + 1) // 2
            src = ysend.at[which, side]
            dst = yrecv.at[which, side, dx + 1]
        return pltpu.make_async_remote_copy(
            src_ref=src,
            dst_ref=dst,
            send_sem=send_sem.at[which, at],
            recv_sem=recv_sem.at[which, at],
            device_id=(span + dx, depth + dy),
            device_id_type=MESH,
        )

    def fill_own(which, row_of):
        buffer = buffers[which]
        for c in range(comps):
            for x in range(width_x):
                buffer[c, rim + x, :, own] = row_of(c, x)
            for side, start in ((0, 128), (1, width_y)):
                edge = buffer[c, pl.ds(rim, width_x), :, pl.ds(start, 128)]
                turned = edge.reshape(width_x * layers, 128).T
                ysend[which, side, c] = turned[:8] if side == 0 else turned[120:]

    def edges_zero(which):
        buffer = buffers[which]
        for dx, start in ((1, 0), (-1, width_x + rim)):

            @pl.when(jnp.logical_not(has(-dx, 0)))
            def _(start=start):
                buffer[:, pl.ds(start, rim), :, own] = jnp.zeros(
                    (comps, rim, layers, width_y), F32
                )

    fill_own(0, lambda c, x: solid[:, x, :] if c == 0 else drag[c - 1, :, x, :])
    edges_zero(0)
    edges_zero(1)
    count = sum(has(dx, dy).astype(jnp.int32) for dx, dy in NEAR)
    pl.semaphore_wait(barrier, count)
    for which in range(2):
        if which == 1:
            fill_own(1, lambda c, x: target[c, x])
        for at, (dx, dy) in enumerate(NEAR):

            @pl.when(has(dx, dy))
            def _(at=at, which=which):
                copy_of(which, at).start()

    def pads(which):
        buffer = buffers[which]
        for at, (dx, dy) in enumerate(NEAR):
            if dy == 0:

                @pl.when(has(-dx, 0))
                def _(at=at):
                    copy_of(which, at).wait_recv()

                continue
            side = (dy + 1) // 2
            lanes = pl.ds(128 + width_y, 128) if side == 0 else pl.ds(0, 128)
            if dx == 0:
                rows, taken = pl.ds(rim, width_x), slice(0, width_x)
            elif dx == 1:
                rows, taken = pl.ds(0, rim), slice(width_x - rim, width_x)
            else:
                rows, taken = pl.ds(width_x + rim, rim), slice(0, rim)

            @pl.when(has(-dx, -dy))
            def _(at=at, side=side, lanes=lanes, rows=rows, taken=taken, dx=dx):
                copy_of(which, at).wait_recv()
                for c in range(comps):
                    block = yrecv[which, side, dx + 1, c]
                    rest = jnp.zeros((120, 128), F32)
                    parts = [block, rest] if side == 0 else [rest, block]
                    turned = jnp.concatenate(parts, axis=0).T.reshape(width_x, layers, 128)
                    buffer[c, rows, :, lanes] = turned[taken]

            @pl.when(jnp.logical_not(has(-dx, -dy)))
            def _(lanes=lanes, rows=rows, taken=taken):
                n = taken.stop - taken.start
                buffer[:, rows, :, lanes] = jnp.zeros((comps, n, layers, 128), F32)

    def sent(which):
        for at, (dx, dy) in enumerate(NEAR):

            @pl.when(has(dx, dy))
            def _(at=at):
                copy_of(which, at).wait_send()

    pads(0)
    pads(1)
    sent(0)
    lane = lax.broadcasted_iota(jnp.int32, (layers, width_y + 256), 1)
    first = jnp.where(depth > 0, 0, 128)
    end = jnp.where(depth < depth_size - 1, width_y + 256, width_y + 128)
    scale = jnp.where((lane >= first) & (lane < end), 1.0 / (1.0 + 4.0 * NU_WEIGHT), 0.0)
    first_row = jnp.where(span > 0, 0, rim)
    end_row = jnp.where(span < span_size - 1, total_x, width_x + rim)
    for c in range(comps):
        for sweep in range(1, SWEEPS + 1):

            def row_step(x, before, c=c):
                here = smooth[c, x]
                beside = before + smooth[c, x + 1]
                beside = beside + pltpu.roll(here, 1, 1) + pltpu.roll(here, width_y + 255, 1)
                inside = jnp.where((x >= first_row) & (x < end_row), 1.0, 0.0)
                smooth[c, x] = (source[c, x] + NU_WEIGHT * beside) * (scale * inside)
                return here

            lax.fori_loop(sweep, total_x - sweep, row_step, smooth[c, sweep - 1], unroll=2)
        out[c] = smooth[c, pl.ds(rim, width_x), :, own]
    sent(1)


VMEM = pl.BlockSpec(memory_space=pltpu.VMEM)
SMEM = pl.BlockSpec(memory_space=pltpu.SMEM)
LIMIT = pltpu.CompilerParams(vmem_limit_bytes=48 * 1024 * 1024)


def on_device(part_slab, part_cell, part_volume, part_drag, part_count, prior_solid, prior_drag):
    span_size = lax.axis_size("span")
    part_rows = part_cell.shape[1]
    cap = 2 * part_rows // span_size
    layers, width_x, width_y = prior_solid.shape
    cols = min(256, cap)
    lines = span_size * cap // cols
    block = math.gcd(part_rows, 512)
    packed, slots = pl.pallas_call(
        functools.partial(pack_kernel, span_size, cap, block),
        out_shape=(
            jax.ShapeDtypeStruct((5, lines, cols), F32),
            jax.ShapeDtypeStruct((1, part_rows), jnp.int32),
        ),
        in_specs=[SMEM] + [VMEM] * 4,
        out_specs=(VMEM, VMEM),
        compiler_params=LIMIT,
        name="pack",
    )(part_count, part_slab.reshape(1, part_rows), part_cell, part_volume, part_drag)
    per = lines // span_size
    recv = lax.all_to_all(
        packed.reshape(5, span_size, per, cols), "span", split_axis=1, concat_axis=1, tiled=True
    ).reshape(5, lines, cols)
    grid_rows = layers * width_x
    target = pl.pallas_call(
        functools.partial(deposit_kernel, 8, layers),
        out_shape=jax.ShapeDtypeStruct((4, grid_rows, width_y), F32),
        in_specs=[VMEM],
        out_specs=VMEM,
        compiler_params=LIMIT,
        name="deposit",
    )(recv)
    target = target.reshape(4, width_x, layers, width_y)
    rim = SWEEPS
    wide = (4, width_x + 2 * rim, layers, width_y + 256)
    smooth = pl.pallas_call(
        functools.partial(sweeps_kernel, rim),
        out_shape=jax.ShapeDtypeStruct(target.shape, F32),
        in_specs=[VMEM] * 3,
        out_specs=VMEM,
        scratch_shapes=[
            pltpu.VMEM(wide, F32),
            pltpu.VMEM(wide, F32),
            pltpu.VMEM((2, 2, 4, 8, 128), F32),
            pltpu.VMEM((2, 2, 3, 4, 8, 128), F32),
            pltpu.SemaphoreType.DMA((2, 8)),
            pltpu.SemaphoreType.DMA((2, 8)),
        ],
        compiler_params=pltpu.CompilerParams(
            vmem_limit_bytes=48 * 1024 * 1024, collective_id=0, has_side_effects=True
        ),
        name="sweeps",
    )(prior_solid, prior_drag, target)
    fields, values = pl.pallas_call(
        functools.partial(gather_kernel, 8),
        out_shape=(
            jax.ShapeDtypeStruct((4, layers, width_x, width_y), F32),
            jax.ShapeDtypeStruct((4, lines, cols), F32),
        ),
        in_specs=[VMEM] * 2,
        out_specs=(VMEM, VMEM),
        scratch_shapes=[pltpu.VMEM((4 * grid_rows, width_y), BF)] * 2,
        compiler_params=LIMIT,
        name="gather",
    )(smooth, recv)
    returned = lax.all_to_all(
        values.reshape(4, span_size, per, cols), "span", split_axis=1, concat_axis=1, tiled=True
    ).reshape(4, lines, cols)
    feedback = pl.pallas_call(
        functools.partial(unpack_kernel, block),
        out_shape=jax.ShapeDtypeStruct((4, 1, part_rows), F32),
        in_specs=[VMEM] * 2,
        out_specs=VMEM,
        compiler_params=LIMIT,
        name="unpack",
    )(returned, slots)
    return (fields, feedback)


def solution(mesh):
    in_specs = (
        P("depth", "span", None),
        P("depth", "span"),
        P("depth", "span"),
        P(None, "depth", "span"),
        P("depth", "span"),
        P(None, "span", "depth"),
        P(None, None, "span", "depth"),
    )
    out_specs = (P(None, None, "span", "depth"), P(None, "depth", "span"))
    return jax.shard_map(
        on_device, mesh=mesh, in_specs=in_specs, out_specs=out_specs, check_vma=False
    )
```

```python
import functools
import math

import jax
import jax.numpy as jnp
from jax import lax
from jax.experimental import pallas as pl
from jax.experimental.pallas import tpu as pltpu
from jax.sharding import PartitionSpec as P

SWEEPS = 6
NU_WEIGHT = 1.0
PHI_LIMIT = 0.6
BF = jnp.bfloat16
F32 = jnp.float32


def two_parts(value):
    high = value.astype(BF)
    return high, (value - high.astype(F32)).astype(BF)


def hot_of(index, count):
    rows = lax.broadcasted_iota(jnp.int32, (count, index.shape[1]), 0)
    return jnp.where(rows == index, 1.0, 0.0).astype(BF)


def nt_dot(left, right):
    return lax.dot_general(left, right, (((1,), (1,)), ((), ())), preferred_element_type=F32)


def spread(values, row, col, rows, cols):
    mask = lax.broadcasted_iota(jnp.int32, (rows, row.shape[1]), 0) == row
    hot = hot_of(col, cols)
    total = None
    for part in range(2):
        left = jnp.concatenate(
            [jnp.where(mask, two_parts(v)[part].astype(F32), 0.0).astype(BF) for v in values], axis=0
        )
        term = nt_dot(left, hot)
        total = term if total is None else total + term
    return total


def pick(high, low, row, col, rows, cols):
    hot = hot_of(col, cols)
    wide = jnp.dot(high, hot, preferred_element_type=F32)
    wide = wide + jnp.dot(low, hot, preferred_element_type=F32)
    mask = lax.broadcasted_iota(jnp.int32, (rows, row.shape[1]), 0) == row
    comps = high.shape[0] // rows
    found = [
        jnp.sum(jnp.where(mask, wide[c * rows : (c + 1) * rows], 0.0), axis=0, keepdims=True)
        for c in range(comps)
    ]
    return found


def pack_kernel(span, cap, block, count, slab, cell, volume, drag, out, slots):
    rows, cols = out.shape[1:]
    part_rows = slab.shape[1]
    out[...] = jnp.zeros_like(out)
    before_lane = lax.broadcasted_iota(jnp.int32, (block, block), 0)
    this_lane = lax.broadcasted_iota(jnp.int32, (block, block), 1)
    tri = jnp.where(before_lane < this_lane, 1.0, 0.0).astype(BF)
    live_count = count[0, 0]

    def step(b, offset):
        lanes = pl.ds(pl.multiple_of(b * block, block), block)
        sl = slab[:, lanes]
        live = b * block + lax.broadcasted_iota(jnp.int32, (1, block), 1) < live_count
        key = jnp.where(live, sl, -1)
        member = jnp.where(lax.broadcasted_iota(jnp.int32, (span, block), 0) == key, 1.0, 0.0)
        before = jnp.dot(member.astype(BF), tri, preferred_element_type=F32)
        place = jnp.sum(member * (before + offset), axis=0, keepdims=True).astype(jnp.int32)
        slot = jnp.where(live, sl * cap + place, -1)
        slots[:, lanes] = slot
        row = lax.shift_right_arithmetic(slot, int(math.log2(cols)))
        col = lax.bitwise_and(slot, cols - 1)
        values = [cell[:, lanes].astype(F32), volume[:, lanes]]
        values += [drag[c, :, lanes] for c in range(drag.shape[0])]
        out[...] += spread(values, row, col, rows, cols).reshape(out.shape)
        return offset + jnp.sum(member, axis=1, keepdims=True)

    lax.fori_loop(0, part_rows // block, step, jnp.zeros((span, 1), F32))


def x_major(ids, layers, width_x, cols):
    line = lax.shift_right_arithmetic(ids, int(math.log2(cols)))
    layer = lax.shift_right_arithmetic(line, int(math.log2(width_x)))
    return lax.bitwise_and(line, width_x - 1) * layers + layer


def deposit_kernel(group, layers, recv, out):
    comps, rows, cols = out.shape
    out[...] = jnp.zeros_like(out)

    def step(g, carry):
        lines = pl.ds(pl.multiple_of(g * group, group), group)
        block = [recv[c, lines, :] for c in range(comps + 1)]
        flat = [
            jnp.concatenate([b[j : j + 1] for j in range(group)], axis=1) for b in block
        ]
        ids = flat[0].astype(jnp.int32)
        row = x_major(ids, layers, rows // layers, cols)
        col = lax.bitwise_and(ids, cols - 1)
        out[...] += spread(flat[1:], row, col, rows, cols).reshape(out.shape)
        return carry

    lax.fori_loop(0, recv.shape[1] // group, step, 0)
    out[0] = jnp.minimum(out[0], PHI_LIMIT)


def gather_kernel(group, smooth, ids_ref, fields, out, high, low):
    comps, width_x, layers, cols = smooth.shape
    rows = width_x * layers
    for x in range(width_x):
        void = 1.0 - smooth[0, x]
        for c in range(comps):
            value = void if c == 0 else -smooth[c, x] / void
            fields[c, :, x, :] = value
            lines = pl.ds(c * rows + x * layers, layers)
            high[lines], low[lines] = two_parts(value)

    def step(g, carry):
        lines = pl.ds(pl.multiple_of(g * group, group), group)
        block = ids_ref[0, lines, :].astype(jnp.int32)
        found = []
        for j in range(group):
            ids = block[j : j + 1]
            row = x_major(ids, layers, width_x, cols)
            col = lax.bitwise_and(ids, cols - 1)
            found.append(pick(high[...], low[...], row, col, rows, cols))
        for c in range(comps):
            out[c, lines, :] = jnp.concatenate([f[c] for f in found], axis=0)
        return carry

    lax.fori_loop(0, ids_ref.shape[1] // group, step, 0)


def unpack_kernel(block, table_ref, slots, out):
    comps, rows, cols = table_ref.shape
    high, low = two_parts(table_ref[...].reshape(comps * rows, cols))

    def step(b, carry):
        lanes = pl.ds(pl.multiple_of(b * block, block), block)
        slot = slots[:, lanes]
        row = lax.shift_right_arithmetic(slot, int(math.log2(cols)))
        col = lax.bitwise_and(slot, cols - 1)
        found = pick(high, low, row, col, rows, cols)
        for c in range(comps):
            out[c, :, lanes] = found[c]
        return carry

    lax.fori_loop(0, slots.shape[1] // block, step, 0)


MESH = pl.DeviceIdType.MESH
NEAR = [(dx, dy) for dx in (-1, 0, 1) for dy in (-1, 0, 1) if (dx, dy) != (0, 0)]


def exchange_kernel(count, data, out, send_sem, recv_sem, own_sem):
    span, depth = lax.axis_index("span"), lax.axis_index("depth")
    barrier = pltpu.get_barrier_semaphore()
    for k in range(1, count):
        to = lax.rem(span + k, count)
        pl.semaphore_signal(barrier, inc=1, device_id=(to, depth), device_id_type=MESH)
    own = pltpu.make_async_copy(data.at[:, span], out.at[:, span], own_sem)
    own.start()
    pl.semaphore_wait(barrier, count - 1)
    copies = []
    for k in range(1, count):
        to = lax.rem(span + k, count)
        copies.append(
            pltpu.make_async_remote_copy(
                src_ref=data.at[:, to],
                dst_ref=out.at[:, span],
                send_sem=send_sem.at[k],
                recv_sem=recv_sem.at[k],
                device_id=(to, depth),
                device_id_type=MESH,
            )
        )
        copies[-1].start()
    own.wait()
    for copy in copies:
        copy.wait()


def exchange(data, number):
    count = data.shape[1]
    return pl.pallas_call(
        functools.partial(exchange_kernel, count),
        out_shape=jax.ShapeDtypeStruct(data.shape, F32),
        in_specs=[VMEM],
        out_specs=VMEM,
        scratch_shapes=[
            pltpu.SemaphoreType.DMA((count,)),
            pltpu.SemaphoreType.DMA((count,)),
            pltpu.SemaphoreType.DMA,
        ],
        compiler_params=pltpu.CompilerParams(
            vmem_limit_bytes=16 * 1024 * 1024, collective_id=number, has_side_effects=True
        ),
        name=f"exchange_{number}",
    )(data)


def sweeps_kernel(
    rim, solid, drag, above, below, target, out, smooth, source, ysend, yrecv, send_sem, recv_sem
):
    comps, width_x, layers, width_y = target.shape
    span, depth = lax.axis_index("span"), lax.axis_index("depth")
    span_size, depth_size = lax.axis_size("span"), lax.axis_size("depth")
    own = pl.ds(128, width_y)
    total_x = width_x + 2 * rim

    def has(dx, dy):
        x, y = span + dx, depth + dy
        return (x >= 0) & (x < span_size) & (y >= 0) & (y < depth_size)

    barrier = pltpu.get_barrier_semaphore()
    for dx, dy in NEAR:

        @pl.when(has(dx, dy))
        def _(dx=dx, dy=dy):
            pl.semaphore_signal(
                barrier, inc=1, device_id=(span + dx, depth + dy), device_id_type=MESH
            )

    buffers = (smooth, source)

    def copy_of(c, which, at):
        dx, dy = NEAR[at]
        width = rim - which
        buffer = buffers[which]
        if dy == 0 and dx == 1:
            src = buffer.at[c, pl.ds(width_x + rim - width, width), :, own]
            dst = buffer.at[c, pl.ds(rim - width, width), :, own]
        elif dy == 0:
            src = buffer.at[c, pl.ds(rim, width), :, own]
            dst = buffer.at[c, pl.ds(width_x + rim, width), :, own]
        else:
            side = (dy + 1) // 2
            src = ysend.at[which, side, c]
            dst = yrecv.at[which, side, dx + 1, c]
        return pltpu.make_async_remote_copy(
            src_ref=src,
            dst_ref=dst,
            send_sem=send_sem.at[c, which, at],
            recv_sem=recv_sem.at[c, which, at],
            device_id=(span + dx, depth + dy),
            device_id_type=MESH,
        )

    def sides(which):
        return [(at, d) for at, d in enumerate(NEAR) if which == 1 or d[1] != 0]

    def fill_own(c, which, row_of):
        buffer = buffers[which]
        for x in range(width_x):
            buffer[c, rim + x, :, own] = row_of(x)
        for side, start in ((0, 128), (1, width_y)):
            edge = buffer[c, pl.ds(rim, width_x), :, pl.ds(start, 128)]
            turned = edge.reshape(width_x * layers, 128).T
            ysend[which, side, c] = turned[:8] if side == 0 else turned[120:]

    for c in range(comps):
        fill_own(c, 1, lambda x: target[c, x])
        fill_own(c, 0, lambda x: solid[:, x, :] if c == 0 else drag[c - 1, :, x, :])
    count = sum(has(dx, dy).astype(jnp.int32) for dx, dy in NEAR)
    pl.semaphore_wait(barrier, count)
    for c in range(comps):
        for which in range(2):
            for at, (dx, dy) in sides(which):

                @pl.when(has(dx, dy))
                def _(c=c, at=at, which=which):
                    copy_of(c, which, at).start()

    for c in range(comps):
        for r in range(rim):
            smooth[c, r, :, own] = above[c, :, r, :]
            smooth[c, width_x + rim + r, :, own] = below[c, :, r, :]
    for dx, start in ((1, 0), (-1, width_x + rim)):

        @pl.when(jnp.logical_not(has(-dx, 0)))
        def _(start=start):
            source[:, pl.ds(start, rim), :, own] = jnp.zeros((comps, rim, layers, width_y), F32)

    def pads(c, which):
        buffer = buffers[which]
        for at, (dx, dy) in sides(which):
            if dy == 0:

                @pl.when(has(-dx, 0))
                def _(at=at):
                    copy_of(c, which, at).wait_recv()

                continue
            side = (dy + 1) // 2
            lanes = pl.ds(128 + width_y, 128) if side == 0 else pl.ds(0, 128)
            if dx == 0:
                rows, taken = pl.ds(rim, width_x), slice(0, width_x)
            elif dx == 1:
                rows, taken = pl.ds(0, rim), slice(width_x - rim, width_x)
            else:
                rows, taken = pl.ds(width_x + rim, rim), slice(0, rim)

            @pl.when(has(-dx, -dy))
            def _(at=at, side=side, lanes=lanes, rows=rows, taken=taken, dx=dx):
                copy_of(c, which, at).wait_recv()
                block = yrecv[which, side, dx + 1, c]
                rest = jnp.zeros((120, 128), F32)
                parts = [block, rest] if side == 0 else [rest, block]
                turned = jnp.concatenate(parts, axis=0).T.reshape(width_x, layers, 128)
                buffer[c, rows, :, lanes] = turned[taken]

            @pl.when(jnp.logical_not(has(-dx, -dy)))
            def _(lanes=lanes, rows=rows, taken=taken):
                n = taken.stop - taken.start
                buffer[c, rows, :, lanes] = jnp.zeros((n, layers, 128), F32)

    def sent(c, which):
        for at, (dx, dy) in sides(which):

            @pl.when(has(dx, dy))
            def _(at=at):
                copy_of(c, which, at).wait_send()

    lane = lax.broadcasted_iota(jnp.int32, (layers, width_y + 256), 1)
    first = jnp.where(depth > 0, 0, 128)
    end = jnp.where(depth < depth_size - 1, width_y + 256, width_y + 128)
    scale = jnp.where((lane >= first) & (lane < end), 1.0 / (1.0 + 4.0 * NU_WEIGHT), 0.0)
    first_row = jnp.where(span > 0, 0, rim)
    end_row = jnp.where(span < span_size - 1, total_x, width_x + rim)
    for c in range(comps):
        pads(c, 0)
        pads(c, 1)
        for sweep in range(1, SWEEPS + 1):

            def row_step(x, before, c=c):
                here = smooth[c, x]
                beside = before + smooth[c, x + 1]
                beside = beside + pltpu.roll(here, 1, 1) + pltpu.roll(here, width_y + 255, 1)
                inside = jnp.where((x >= first_row) & (x < end_row), 1.0, 0.0)
                smooth[c, x] = (source[c, x] + NU_WEIGHT * beside) * (scale * inside)
                return here

            lax.fori_loop(sweep, total_x - sweep, row_step, smooth[c, sweep - 1], unroll=2)
        out[c] = smooth[c, pl.ds(rim, width_x), :, own]
    for c in range(comps):
        sent(c, 0)
        sent(c, 1)


VMEM = pl.BlockSpec(memory_space=pltpu.VMEM)
SMEM = pl.BlockSpec(memory_space=pltpu.SMEM)
LIMIT = pltpu.CompilerParams(vmem_limit_bytes=48 * 1024 * 1024)


def on_device(part_slab, part_cell, part_volume, part_drag, part_count, prior_solid, prior_drag):
    span_size = lax.axis_size("span")
    part_rows = part_cell.shape[1]
    cap = 2 * part_rows // span_size
    layers, width_x, width_y = prior_solid.shape
    cols = min(256, cap)
    lines = span_size * cap // cols
    block = math.gcd(part_rows, 512)
    rim = SWEEPS
    up = [(i, i + 1) for i in range(span_size - 1)]
    down = [(j, i) for i, j in up]
    edge = jnp.concatenate([prior_solid[None, :, -rim:], prior_drag[:, :, -rim:]], axis=0)
    above = lax.ppermute(edge, "span", up)
    edge = jnp.concatenate([prior_solid[None, :, :rim], prior_drag[:, :, :rim]], axis=0)
    below = lax.ppermute(edge, "span", down)
    packed, slots = pl.pallas_call(
        functools.partial(pack_kernel, span_size, cap, block),
        out_shape=(
            jax.ShapeDtypeStruct((5, lines, cols), F32),
            jax.ShapeDtypeStruct((1, part_rows), jnp.int32),
        ),
        in_specs=[SMEM] + [VMEM] * 4,
        out_specs=(VMEM, VMEM),
        compiler_params=LIMIT,
        name="pack",
    )(part_count, part_slab.reshape(1, part_rows), part_cell, part_volume, part_drag)
    per = lines // span_size
    recv = exchange(packed.reshape(5, span_size, per, cols), 1).reshape(5, lines, cols)
    grid_rows = layers * width_x
    target = pl.pallas_call(
        functools.partial(deposit_kernel, 8, layers),
        out_shape=jax.ShapeDtypeStruct((4, grid_rows, width_y), F32),
        in_specs=[VMEM],
        out_specs=VMEM,
        compiler_params=LIMIT,
        name="deposit",
    )(recv)
    target = target.reshape(4, width_x, layers, width_y)
    wide = (4, width_x + 2 * rim, layers, width_y + 256)
    smooth = pl.pallas_call(
        functools.partial(sweeps_kernel, rim),
        out_shape=jax.ShapeDtypeStruct(target.shape, F32),
        in_specs=[VMEM] * 5,
        out_specs=VMEM,
        scratch_shapes=[
            pltpu.VMEM(wide, F32),
            pltpu.VMEM(wide, F32),
            pltpu.VMEM((2, 2, 4, 8, 128), F32),
            pltpu.VMEM((2, 2, 3, 4, 8, 128), F32),
            pltpu.SemaphoreType.DMA((4, 2, 8)),
            pltpu.SemaphoreType.DMA((4, 2, 8)),
        ],
        compiler_params=pltpu.CompilerParams(
            vmem_limit_bytes=48 * 1024 * 1024, collective_id=0, has_side_effects=True
        ),
        name="sweeps",
    )(prior_solid, prior_drag, above, below, target)
    fields, values = pl.pallas_call(
        functools.partial(gather_kernel, 8),
        out_shape=(
            jax.ShapeDtypeStruct((4, layers, width_x, width_y), F32),
            jax.ShapeDtypeStruct((4, lines, cols), F32),
        ),
        in_specs=[VMEM] * 2,
        out_specs=(VMEM, VMEM),
        scratch_shapes=[pltpu.VMEM((4 * grid_rows, width_y), BF)] * 2,
        compiler_params=LIMIT,
        name="gather",
    )(smooth, recv)
    returned = exchange(values.reshape(4, span_size, per, cols), 2).reshape(4, lines, cols)
    feedback = pl.pallas_call(
        functools.partial(unpack_kernel, block),
        out_shape=jax.ShapeDtypeStruct((4, 1, part_rows), F32),
        in_specs=[VMEM] * 2,
        out_specs=VMEM,
        compiler_params=LIMIT,
        name="unpack",
    )(returned, slots)
    return (fields, feedback)


def solution(mesh):
    in_specs = (
        P("depth", "span", None),
        P("depth", "span"),
        P("depth", "span"),
        P(None, "depth", "span"),
        P("depth", "span"),
        P(None, "span", "depth"),
        P(None, None, "span", "depth"),
    )
    out_specs = (P(None, None, "span", "depth"), P(None, "depth", "span"))
    return jax.shard_map(
        on_device, mesh=mesh, in_specs=in_specs, out_specs=out_specs, check_vma=False
    )
```
